32 devices in a mesh: xy: 2 (over core), gz: 4 (over y, x), ta: 4 (over z).
Axes of the slice: x: 2, y: 2, z: 4, core: 2. Of those that a mesh axis runs over, the one named last changes fastest.
Arguments:
- right_side: float32 [2, 4, 4, 128, 128], P('xy', 'gz', 'ta'), may hold values from -40 to 40
- link_blocks: float32 [2, 4, 4, 9, 2, 32, 32, 128], P('xy', 'gz', 'ta'), may hold values from -0.75 to 0.75
Outputs:
- solution: float32 [2, 4, 4, 128, 128], P('xy', 'gz', 'ta')
- residual: float32 [2, 4, 4, 128, 128], P('xy', 'gz', 'ta')
The draws below stay inside these ranges and needn't reach their ends.
All inputs are finite; a program needn't handle non-finite values.
Results may differ from the reference program's by a relative error of at most 0.00018.
Values sent between devices are 32-bit elements; how exact they have to be, the bound alone decides.
A program may use at most 128 MiB of HBM per device.

```python
import jax
import jax.numpy as jnp
from jax import lax

DOF = 32
RHS = 2
CX = 1
NY = 8
CZ = 2
CT = 8
ITERS = 2
S = 128
VEC = 128
NT = 32
N_XY = 2
N_GZ = 4
N_TA = 4


def draw_right_side(key, part):
    noise_key, rough_key = jax.random.split(jax.random.fold_in(key, 11), 2)
    shape = (N_XY, N_GZ, N_TA, S, VEC)
    time_index = (jnp.arange(N_TA)[:, None] * CT + jnp.arange(S)[None, :] % CT).astype(jnp.float32)
    ramp = jnp.exp(jnp.log(3.0) * time_index / max(NT - 1, 1))
    ramp = ramp[None, None, :, :, None]
    rough = jnp.exp(jax.random.uniform(rough_key, (N_XY, N_GZ, N_TA, S, 1), jnp.float32, -0.8, 0.8))
    base = jax.random.normal(noise_key, shape, jnp.float32)
    return jnp.clip(base * ramp * rough, -40.0, 40.0).astype(jnp.float32)


def steps_of(stream_key, dims, cuts, smallest, largest):
    gain = 1.0
    for position, shards_of in cuts:
        steps = jax.random.uniform(jax.random.fold_in(jax.random.fold_in(stream_key, 6), position), (shards_of,), jnp.float32, smallest / len(cuts), largest / len(cuts))
        gain = gain * jnp.repeat(jnp.exp(steps), dims[position] // shards_of).reshape((-1,) + (1,) * (len(dims) - 1 - position))
    return gain


def gaussian(stream_key, dims, spread, reach, shards=(), held_as=jnp.bfloat16):
    factor_of = steps_of(stream_key, dims, shards, -0.22, 0.18) if shards else 1.0
    drawn = jax.random.normal(stream_key, dims, jnp.float32) * spread * factor_of
    return jnp.minimum(jnp.maximum(drawn, -reach), reach).astype(held_as)


def setup_inputs(seed: int = 0) -> dict:
    arg_keys = jax.random.split(jax.random.key(seed), 3)
    right_side = draw_right_side(jax.random.fold_in(arg_keys[2], 71), 0)
    link_blocks = gaussian(arg_keys[1], (N_XY, N_GZ, N_TA, 9, 2, DOF, DOF, S), (2 * DOF) ** -0.5, 0.75, ((0, 2), (1, 4), (2, 4)), jnp.float32)
    return dict(right_side=right_side, link_blocks=link_blocks)


mass_shift = 4.0
epsilon = 1e-06

def split_parts(joined):
    shaped = joined.reshape(joined.shape[:-1] + (RHS, 2, DOF))
    return (shaped[..., 0, :], shaped[..., 1, :])

def join_parts(real, imaginary):
    stacked = jnp.stack((real, imaginary), -2)
    return stacked.reshape(stacked.shape[:-3] + (-1,))

def column_sums(values):
    folded = lax.optimization_barrier(jnp.sum(values, axis=-1))
    return lax.optimization_barrier(jnp.sum(folded.reshape(-1, folded.shape[-1]), axis=0))

def to_lattice(joined):
    shaped = joined.reshape(N_XY, N_GZ, N_TA, CX, NY, CZ, CT, joined.shape[-1])
    moved = jnp.transpose(shaped, (0, 3, 4, 1, 5, 2, 6, 7))
    return moved.reshape(N_XY * CX, NY, N_GZ * CZ, N_TA * CT, joined.shape[-1])

def to_blocks(lattice):
    shaped = lattice.reshape(N_XY, CX, NY, N_GZ, CZ, N_TA, CT, lattice.shape[-1])
    moved = jnp.transpose(shaped, (0, 3, 5, 1, 2, 4, 6, 7))
    return moved.reshape(N_XY, N_GZ, N_TA, CX * NY * CZ * CT, lattice.shape[-1])

def single(blocks, field):
    return jnp.einsum('...cds,...srd->...src', blocks, field, precision=lax.Precision.HIGHEST)

def apply_operator(link_blocks, real, imaginary):
    lattice = to_lattice(join_parts(real, imaginary))
    shifted_operator = [lattice]
    for axis_number in range(4):
        shifted_operator.append(jnp.roll(lattice, -1, axis_number))
        shifted_operator.append(jnp.roll(lattice, 1, axis_number))
    out_real = mass_shift * real
    output_imaginary = mass_shift * imaginary
    for level in range(9):
        near_real, near_imag = split_parts(to_blocks(shifted_operator[level]))
        blocks_real = link_blocks[:, :, :, level, 0]
        blocks_imag = link_blocks[:, :, :, level, 1]
        out_real = out_real + single(blocks_real, near_real) - single(blocks_imag, near_imag)
        output_imaginary = output_imaginary + single(blocks_real, near_imag) + single(blocks_imag, near_real)
    return (out_real, output_imaginary)

def solve_positive_definite(matrix, target):
    size = matrix.shape[0]
    lower = {}
    for row in range(size):
        for col in range(row + 1):
            value = matrix[row, col]
            for inner in range(col):
                value = value - lower[row, inner] * lower[col, inner]
            if row == col:
                lower[row, row] = jnp.sqrt(value)
            else:
                lower[row, col] = value / lower[col, col]
    forward = []
    for row in range(size):
        value = target[row]
        for inner in range(row):
            value = value - lower[row, inner] * forward[inner]
        forward.append(value / lower[row, row])
    answer = [None] * size
    for row in reversed(range(size)):
        value = forward[row]
        for inner in range(row + 1, size):
            value = value - lower[inner, row] * answer[inner]
        answer[row] = value / lower[row, row]
    return jnp.stack(answer)

def least_squares(hessenberg_real, hessenberg_imaginary, beta):
    exact_answer_vector = lax.Precision.HIGHEST
    gram_matrix_real = jnp.einsum('sxm,szm->xzm', hessenberg_real, hessenberg_real, precision=exact_answer_vector) + jnp.einsum('sxm,szm->xzm', hessenberg_imaginary, hessenberg_imaginary, precision=exact_answer_vector)
    gram_matrix_imaginary = jnp.einsum('sxm,szm->xzm', hessenberg_real, hessenberg_imaginary, precision=exact_answer_vector) - jnp.einsum('sxm,szm->xzm', hessenberg_imaginary, hessenberg_real, precision=exact_answer_vector)
    upper = jnp.concatenate((gram_matrix_real, -gram_matrix_imaginary), 1)
    bottom = jnp.concatenate((gram_matrix_imaginary, gram_matrix_real), 1)
    system = jnp.concatenate((upper, bottom), 0)
    target = jnp.concatenate((beta[None, :] * hessenberg_real[0], -beta[None, :] * hessenberg_imaginary[0]), 0)
    answer = solve_positive_definite(system, target)
    return (answer[:ITERS], answer[ITERS:])

def reference(right_side, link_blocks):
    rhs_real, rhs_imag = split_parts(right_side)
    beta = jnp.sqrt(column_sums(rhs_real * rhs_real + rhs_imag * rhs_imag) + epsilon)
    basis = [(rhs_real / beta[:, None], rhs_imag / beta[:, None])]
    hessenberg_real = jnp.zeros((ITERS + 1, ITERS, RHS), jnp.float32)
    hessenberg_imaginary = jnp.zeros((ITERS + 1, ITERS, RHS), jnp.float32)
    for step in range(ITERS):
        work_real, work_imag = apply_operator(link_blocks, basis[step][0], basis[step][1])
        proj_real = jnp.stack([column_sums(vector[0] * work_real + vector[1] * work_imag) for vector in basis])
        proj_imag = jnp.stack([column_sums(vector[0] * work_imag - vector[1] * work_real) for vector in basis])
        for index in range(len(basis)):
            coef_real = proj_real[index][:, None]
            coef_imag = proj_imag[index][:, None]
            vector = basis[index]
            work_real = work_real - (coef_real * vector[0] - coef_imag * vector[1])
            work_imag = work_imag - (coef_real * vector[1] + coef_imag * vector[0])
        norm = jnp.sqrt(column_sums(work_real * work_real + work_imag * work_imag) + epsilon)
        hessenberg_real = hessenberg_real.at[:step + 1, step].set(proj_real)
        hessenberg_imaginary = hessenberg_imaginary.at[:step + 1, step].set(proj_imag)
        hessenberg_real = hessenberg_real.at[step + 1, step].set(norm)
        basis.append((work_real / norm[:, None], work_imag / norm[:, None]))
    coef_real, coef_imag = least_squares(hessenberg_real, hessenberg_imaginary, beta)
    sol_real = jnp.zeros_like(rhs_real)
    sol_imag = jnp.zeros_like(rhs_imag)
    for index in range(ITERS):
        weight_real = coef_real[index][:, None]
        weight_imag = coef_imag[index][:, None]
        sol_real = sol_real + weight_real * basis[index][0] - weight_imag * basis[index][1]
        sol_imag = sol_imag + weight_real * basis[index][1] + weight_imag * basis[index][0]
    image_real, image_imag = apply_operator(link_blocks, sol_real, sol_imag)
    return (join_parts(sol_real, sol_imag), join_parts(rhs_real - image_real, rhs_imag - image_imag))
```

```python
import functools

import jax
import jax.numpy as jnp
from jax import lax
from jax.experimental import pallas as pl
from jax.experimental.pallas import tpu as pltpu
from jax.sharding import PartitionSpec as P

DOF = 32
RHS = 2
NY = 8
CZ = 2
CT = 8
S = 128
E = 128
MESH = pl.DeviceIdType.MESH

mass_shift = 4.0
epsilon = 1e-06


def cmul(a, b):
    return (a[0] * b[0] - a[1] * b[1], a[0] * b[1] + a[1] * b[0])


def conj(a):
    return (a[0], -a[1])


def cadd(a, b):
    return (a[0] + b[0], a[1] + b[1])


def csub(a, b):
    return (a[0] - b[0], a[1] - b[1])


def scale(a, x):
    return (a[0] * x, a[1] * x)


def size2(a):
    return a[0] * a[0] + a[1] * a[1]


def coefficients(g00, g11, g22, g01, g02, g12):
    beta2 = g00 + epsilon
    beta = jnp.sqrt(beta2)
    inv_beta2 = 1.0 / beta2
    h00 = scale((mass_shift * g00 + g01[0], g01[1]), inv_beta2)
    a = (mass_shift - h00[0], -h00[1])
    left = g11 + size2(a) * g00 + 2.0 * cmul(conj(a), g01)[0]
    h10_2 = jnp.maximum(left, 0.0) * inv_beta2 + epsilon
    h10 = jnp.sqrt(h10_2)
    a4 = (a[0] + mass_shift, a[1])
    a_4 = scale(a, mass_shift)
    top = cadd(cadd(g02, cmul(a4, g01)), scale(a_4, g00))
    h01 = scale(top, inv_beta2 / h10)
    low = cadd(cadd(g12, scale(a4, g11)), cmul(a_4, conj(g01)))
    h11 = scale(cadd(low, cmul(conj(a), top)), inv_beta2 / h10_2)
    p = csub(a4, h11)
    q = csub(csub(a_4, scale(h01, h10)), cmul(h11, a))
    left = g22 + size2(p) * g11 + size2(q) * g00
    left = left + 2.0 * (
        cmul(p, conj(g12))[0] + cmul(q, conj(g02))[0] + cmul(cmul(conj(q), p), g01)[0]
    )
    h21_2 = jnp.maximum(left, 0.0) * (inv_beta2 / h10_2) + epsilon
    m00 = size2(h00) + h10_2
    m01 = cadd(cmul(conj(h00), h01), scale(h11, h10))
    m11 = size2(h01) + size2(h11) + h21_2
    t0 = scale(conj(h00), beta)
    t1 = scale(conj(h01), beta)
    inv_l0 = 1.0 / jnp.sqrt(m00)
    l10 = scale(conj(m01), inv_l0)
    f0 = scale(t0, inv_l0)
    inv_d = 1.0 / (m11 - size2(l10))
    y1 = scale(csub(t1, cmul(l10, f0)), inv_d)
    y0 = scale(csub(f0, cmul(conj(l10), y1)), inv_l0)
    inv_beta = 1.0 / beta
    wb = scale(y1, inv_beta / h10)
    wa = cadd(scale(y0, inv_beta), cmul(wb, a))
    return wa, wb


def kernel(
    sizes, b_hbm, l_hbm, sol_ref, res_ref,
    links, field, xbuf, zbuf, tface, tbuf, turned, acc, part, red1, red2,
    b_sem, l_sem, send_sem, recv_sem, s1_send, s1_recv, s2_send, s2_recv,
):
    nx, nz, nt = sizes
    group = nx * nz
    ix, iz, it = lax.axis_index("xy"), lax.axis_index("gz"), lax.axis_index("ta")
    here = ix * nz + iz

    def step(axis_value, by, count):
        return lax.rem(axis_value + (by + count), count)

    def mate(delta):
        other = lax.rem(here + delta, group)
        return (other // nz, lax.rem(other, nz), it)

    order = [0, 3, 4, 1, 2, 7, 8, 5, 6]
    b_copy = pltpu.make_async_copy(b_hbm.at[0, 0, 0], field.at[0], b_sem)
    b_copy.start()
    l_copies = {}
    for k in order:
        l_copies[k] = pltpu.make_async_copy(l_hbm.at[0, 0, 0, k], links.at[k], l_sem.at[k])
        l_copies[k].start()

    barrier = pltpu.get_barrier_semaphore()
    for delta in range(1, group):
        pl.semaphore_signal(barrier, inc=1, device_id=mate(delta), device_id_type=MESH)
    for delta in range(1, nt):
        pl.semaphore_signal(
            barrier, inc=1, device_id=(ix, iz, step(it, delta, nt)), device_id_type=MESH
        )
    pl.semaphore_wait(barrier, group - 1 + nt - 1)
    b_copy.wait()

    lane = lax.broadcasted_iota(jnp.int32, (S, E), 1)
    in_t = lane % CT
    in_z = (lane // CT) % CZ
    row8 = lax.broadcasted_iota(jnp.int32, (8, 128), 0)

    def halo(n):
        mine = field.at[n]
        tface[n, 0] = field[n, pl.ds(0, NY * CZ, stride=CT), :]
        tface[n, 1] = field[n, pl.ds(CT - 1, NY * CZ, stride=CT), :]
        tiles = mine.reshape(NY, CZ, CT, E)
        moves = []
        for way in (0, 1):
            by = 1 if way else -1
            moves.append(
                ("z%d" % way, tiles.at[:, way * (CZ - 1)], zbuf.at[n].reshape(NY, CZ, CT, E).at[:, (1 - way) * (CZ - 1)],
                 (ix, step(iz, by, nz), it))
            )
        for way in (0, 1):
            by = 1 if way else -1
            moves.append(("t%d" % way, tface.at[n, way], tbuf.at[n, way], (ix, iz, step(it, by, nt))))
        for way in (0, 1) if nx > 2 else (0,):
            by = 1 if way else -1
            moves.append(("x%d" % way, mine, xbuf.at[n, way], (step(ix, by, nx), iz, it)))
        copies = {}
        for number, (name, source, target, device) in enumerate(moves):
            copy = pltpu.make_async_remote_copy(
                src_ref=source, dst_ref=target,
                send_sem=send_sem.at[n, number], recv_sem=recv_sem.at[n, number],
                device_id=device, device_id_type=MESH,
            )
            copy.start()
            copies[name] = copy
        return copies

    def products(ks, fresh, merge, keep):
        def body(c, carry):
            if fresh:
                sums = [jnp.zeros((8, 128), jnp.float32) for _ in range(4)]
            else:
                sums = [acc[i, c] for i in range(4)]
            for k in ks:
                for j in range(DOF // 8):
                    rows = pl.ds(8 * j, 8)
                    lr = links[k, 0, c, rows, :]
                    li = links[k, 1, c, rows, :]
                    if merge:
                        lr = lr + links[k + 1, 0, c, rows, :]
                        li = li + links[k + 1, 1, c, rows, :]
                        if keep:
                            links[k, 0, c, rows, :] = lr
                            links[k, 1, c, rows, :] = li
                    for r in range(RHS):
                        vr = turned[k, pl.ds(2 * r * DOF + 8 * j, 8), :]
                        vi = turned[k, pl.ds((2 * r + 1) * DOF + 8 * j, 8), :]
                        sums[2 * r] = sums[2 * r] + lr * vr - li * vi
                        sums[2 * r + 1] = sums[2 * r + 1] + lr * vi + li * vr
            for i in range(4):
                acc[i, c] = sums[i]
            return carry

        lax.fori_loop(0, DOF, body, 0, unroll=2)

    def fold(xs):
        low = row8 < 4
        ys = [
            jnp.where(low, xs[i], xs[i + 4]) + pltpu.roll(jnp.where(low, xs[i + 4], xs[i]), 4, 0)
            for i in range(4)
        ]
        low = row8 % 4 < 2
        zs = [
            jnp.where(low, ys[i] + pltpu.roll(ys[i], 6, 0), ys[i + 2] + pltpu.roll(ys[i + 2], 2, 0))
            for i in range(2)
        ]
        return jnp.where(
            row8 % 2 < 1, zs[0] + pltpu.roll(zs[0], 7, 0), zs[1] + pltpu.roll(zs[1], 1, 0)
        )

    def apply(n, copies):
        own = turned[0]
        turned[3] = pltpu.roll(own, S - CZ * CT, 1)
        turned[4] = pltpu.roll(own, CZ * CT, 1)
        if n == 0:
            for k in (0, 3, 4):
                l_copies[k].wait()
        products((0, 3, 4), True, False, False)
        turned[5] = pltpu.roll(turned[0], S - CT, 1)
        turned[6] = pltpu.roll(turned[0], CT, 1)
        turned[7] = pltpu.roll(turned[0], S - 1, 1)
        turned[8] = pltpu.roll(turned[0], 1, 1)
        if n == 0:
            for k in (1, 2, 7, 8, 5, 6):
                l_copies[k].wait()
        copies["x0"].wait_recv()
        turned[1] = xbuf[n, 0].T
        if nx > 2:
            copies["x1"].wait_recv()
            turned[2] = xbuf[n, 1].T
            products((1, 2), False, False, False)
        else:
            products((1,), False, n == 0, n == 0)
        copies["t0"].wait_recv()
        copies["t1"].wait_recv()
        edge = field.at[3]
        edge[pl.ds(CT - 1, NY * CZ, stride=CT), :] = tbuf[n, 0]
        edge[pl.ds(0, NY * CZ, stride=CT), :] = tbuf[n, 1]
        edges = edge[...].T
        turned[7] = jnp.where(in_t == CT - 1, edges, turned[7])
        turned[8] = jnp.where(in_t == 0, edges, turned[8])
        copies["z0"].wait_recv()
        copies["z1"].wait_recv()
        edges = zbuf[n].T
        turned[5] = jnp.where(in_z == CZ - 1, edges, turned[5])
        turned[6] = jnp.where(in_z == 0, edges, turned[6])
        products((7, 8, 5, 6), False, False, False)
        for i in range(4):
            for c in range(0, DOF, 8):
                turned[0, pl.ds(i * DOF + c, 8), :] = fold([acc[i, c + j] for j in range(8)])
        field[n + 1] = turned[0].T

    field[3] = jnp.zeros((S, E), jnp.float32)
    first = halo(0)
    turned[0] = field[0].T
    apply(0, first)
    second = halo(1)
    apply(1, second)

    in_p = (lax.broadcasted_iota(jnp.int32, (S, E), 1) // DOF) % 2

    def aside(v):
        return jnp.where(in_p == 0, pltpu.roll(v, E - DOF, 1), -pltpu.roll(v, DOF, 1))

    def total(u, v):
        return jnp.sum((u * v).reshape(S // 8, 8, E), axis=0)

    k0, k1, k2 = field[0], field[1], field[2]
    z1, z2 = aside(k1), aside(k2)
    zero = jnp.zeros((8, 128), jnp.float32)
    sums = [
        total(k0, k0), total(k1, k1), total(k2, k2), total(k0, k1), total(k0, z1),
        total(k0, k2), total(k0, z2), total(k1, k2),
    ]
    part[0] = fold(sums)
    part[1] = fold([total(k1, z2)] + [zero] * 7)

    def exchange(count, target, sends, recvs, device):
        copies = []
        for delta in range(1, count):
            copies.append(
                pltpu.make_async_remote_copy(
                    src_ref=target.at[0], dst_ref=target.at[delta],
                    send_sem=sends.at[delta], recv_sem=recvs.at[delta],
                    device_id=device(delta), device_id_type=MESH,
                )
            )
        for copy in copies:
            copy.start()
        value = target[0]
        for copy in copies:
            copy.wait_recv()
        for delta in range(1, count):
            value = value + target[delta]
        return copies, value

    red1[0] = part[...]
    sent1, value = exchange(group, red1, s1_send, s1_recv, mate)
    red2[0] = value
    sent2, value = exchange(
        nt, red2, s2_send, s2_recv, lambda delta: (ix, iz, step(it, delta, nt))
    )
    value = value.reshape(16, 128)
    half = lax.broadcasted_iota(jnp.int32, (16, 128), 1) < 2 * DOF
    sum0 = jnp.sum(jnp.where(half, value, 0.0), axis=1, keepdims=True)
    sum1 = jnp.sum(jnp.where(half, 0.0, value), axis=1, keepdims=True)
    gram = jnp.where(half, sum0, sum1)
    g = [gram[i : i + 1] for i in range(9)]
    wa, wb = coefficients(g[0], g[1], g[2], (g[3], g[4]), (g[5], g[6]), (g[7], g[8]))

    def weighted(w, v, z):
        return w[0] * v - w[1] * z

    k0, k1, k2 = field[0], field[1], field[2]
    z0, z1, z2 = aside(k0), aside(k1), aside(k2)
    sol = weighted(wa, k0, z0) + weighted(wb, k1, z1)
    image = weighted(wa, k1, z1) + weighted(wb, k2, z2)
    sol_ref[0, 0, 0] = sol
    res_ref[0, 0, 0] = k0 - mass_shift * sol - image
    for copies in (first, second):
        for copy in copies.values():
            copy.wait_send()
    for copy in sent1 + sent2:
        copy.wait_send()


def shards(sizes, right_side, link_blocks):
    nx, nz, nt = sizes
    out = jax.ShapeDtypeStruct(right_side.shape, jnp.float32)
    f32 = jnp.float32
    moves = 6 if nx > 2 else 5
    return pl.pallas_call(
        functools.partial(kernel, sizes),
        out_shape=(out, out),
        in_specs=[pl.BlockSpec(memory_space=pl.ANY)] * 2,
        out_specs=(pl.BlockSpec(memory_space=pltpu.VMEM),) * 2,
        scratch_shapes=[
            pltpu.VMEM((9, 2, DOF, DOF, S), f32),
            pltpu.VMEM((4, S, E), f32),
            pltpu.VMEM((2, 2, S, E), f32),
            pltpu.VMEM((2, S, E), f32),
            pltpu.VMEM((2, 2, NY * CZ, E), f32),
            pltpu.VMEM((2, 2, NY * CZ, E), f32),
            pltpu.VMEM((9, E, S), f32),
            pltpu.VMEM((4, DOF, 8, S), f32),
            pltpu.VMEM((2, 8, 128), f32),
            pltpu.VMEM((nx * nz, 2, 8, 128), f32),
            pltpu.VMEM((nt, 2, 8, 128), f32),
            pltpu.SemaphoreType.DMA,
            pltpu.SemaphoreType.DMA((9,)),
            pltpu.SemaphoreType.DMA((2, moves)),
            pltpu.SemaphoreType.DMA((2, moves)),
            pltpu.SemaphoreType.DMA((nx * nz,)),
            pltpu.SemaphoreType.DMA((nx * nz,)),
            pltpu.SemaphoreType.DMA((nt,)),
            pltpu.SemaphoreType.DMA((nt,)),
        ],
        compiler_params=pltpu.CompilerParams(
            collective_id=0, has_side_effects=True, vmem_limit_bytes=60 * 1024 * 1024
        ),
    )(right_side, link_blocks)


def solution(mesh):
    sizes = tuple(mesh.shape[name] for name in ("xy", "gz", "ta"))
    return jax.shard_map(
        functools.partial(shards, sizes),
        mesh=mesh,
        in_specs=(
            P("xy", "gz", "ta", None, None),
            P("xy", "gz", "ta", None, None, None, None, None),
        ),
        out_specs=(P("xy", "gz", "ta", None, None), P("xy", "gz", "ta", None, None)),
        check_vma=False,
    )
```

```python
import functools

import jax
import jax.numpy as jnp
from jax import lax
from jax.experimental import pallas as pl
from jax.experimental.pallas import tpu as pltpu
from jax.sharding import PartitionSpec as P

DOF = 32
RHS = 2
NY = 8
CZ = 2
CT = 8
S = 128
E = 128
MESH = pl.DeviceIdType.MESH

mass_shift = 4.0
epsilon = 1e-06


def cmul(a, b):
    return (a[0] * b[0] - a[1] * b[1], a[0] * b[1] + a[1] * b[0])


def conj(a):
    return (a[0], -a[1])


def cadd(a, b):
    return (a[0] + b[0], a[1] + b[1])


def csub(a, b):
    return (a[0] - b[0], a[1] - b[1])


def scale(a, x):
    return (a[0] * x, a[1] * x)


def size2(a):
    return a[0] * a[0] + a[1] * a[1]


def coefficients(g00, g11, g22, g01, g02, g12):
    beta2 = g00 + epsilon
    beta = jnp.sqrt(beta2)
    inv_beta2 = 1.0 / beta2
    h00 = scale((mass_shift * g00 + g01[0], g01[1]), inv_beta2)
    a = (mass_shift - h00[0], -h00[1])
    left = g11 + size2(a) * g00 + 2.0 * cmul(conj(a), g01)[0]
    h10_2 = jnp.maximum(left, 0.0) * inv_beta2 + epsilon
    h10 = jnp.sqrt(h10_2)
    a4 = (a[0] + mass_shift, a[1])
    a_4 = scale(a, mass_shift)
    top = cadd(cadd(g02, cmul(a4, g01)), scale(a_4, g00))
    h01 = scale(top, inv_beta2 / h10)
    low = cadd(cadd(g12, scale(a4, g11)), cmul(a_4, conj(g01)))
    h11 = scale(cadd(low, cmul(conj(a), top)), inv_beta2 / h10_2)
    p = csub(a4, h11)
    q = csub(csub(a_4, scale(h01, h10)), cmul(h11, a))
    left = g22 + size2(p) * g11 + size2(q) * g00
    left = left + 2.0 * (
        cmul(p, conj(g12))[0] + cmul(q, conj(g02))[0] + cmul(cmul(conj(q), p), g01)[0]
    )
    h21_2 = jnp.maximum(left, 0.0) * (inv_beta2 / h10_2) + epsilon
    m00 = size2(h00) + h10_2
    m01 = cadd(cmul(conj(h00), h01), scale(h11, h10))
    m11 = size2(h01) + size2(h11) + h21_2
    t0 = scale(conj(h00), beta)
    t1 = scale(conj(h01), beta)
    inv_l0 = 1.0 / jnp.sqrt(m00)
    l10 = scale(conj(m01), inv_l0)
    f0 = scale(t0, inv_l0)
    inv_d = 1.0 / (m11 - size2(l10))
    y1 = scale(csub(t1, cmul(l10, f0)), inv_d)
    y0 = scale(csub(f0, cmul(conj(l10), y1)), inv_l0)
    inv_beta = 1.0 / beta
    wb = scale(y1, inv_beta / h10)
    wa = cadd(scale(y0, inv_beta), cmul(wb, a))
    return wa, wb


def kernel(
    sizes, b_hbm, l_hbm, sol_ref, res_ref,
    links, field, xbuf, zbuf, tface, tbuf, turned, acc, part, red1, red2,
    b_sem, l_sem, send_sem, recv_sem, s1_send, s1_recv, s2_send, s2_recv,
):
    nx, nz, nt = sizes
    group = nx * nz
    ix, iz, it = lax.axis_index("xy"), lax.axis_index("gz"), lax.axis_index("ta")
    here = ix * nz + iz

    def step(axis_value, by, count):
        return lax.rem(axis_value + (by + count), count)

    def mate(delta):
        other = lax.rem(here + delta, group)
        return (other // nz, lax.rem(other, nz), it)

    order = [0, 3, 4, 1, 2, 7, 8, 5, 6]
    b_copy = pltpu.make_async_copy(b_hbm.at[0, 0, 0], field.at[0], b_sem)
    b_copy.start()
    l_copies = {}
    for k in order:
        l_copies[k] = pltpu.make_async_copy(l_hbm.at[0, 0, 0, k], links.at[k], l_sem.at[k])
        l_copies[k].start()

    barrier = pltpu.get_barrier_semaphore()
    for delta in range(1, group):
        pl.semaphore_signal(barrier, inc=1, device_id=mate(delta), device_id_type=MESH)
    for delta in range(1, nt):
        pl.semaphore_signal(
            barrier, inc=1, device_id=(ix, iz, step(it, delta, nt)), device_id_type=MESH
        )
    pl.semaphore_wait(barrier, group - 1 + nt - 1)
    b_copy.wait()

    lane = lax.broadcasted_iota(jnp.int32, (S, E), 1)
    in_t = lane % CT
    in_z = (lane // CT) % CZ
    row8 = lax.broadcasted_iota(jnp.int32, (8, 128), 0)

    def halo(n):
        mine = field.at[n]
        tface[n, 0] = field[n, pl.ds(0, NY * CZ, stride=CT), :]
        tface[n, 1] = field[n, pl.ds(CT - 1, NY * CZ, stride=CT), :]
        tiles = mine.reshape(NY, CZ, CT, E)
        moves = []
        for way in (0, 1):
            by = 1 if way else -1
            moves.append(("t%d" % way, tface.at[n, way], tbuf.at[n, way], (ix, iz, step(it, by, nt))))
        for way in (0, 1):
            by = 1 if way else -1
            moves.append(
                ("z%d" % way, tiles.at[:, way * (CZ - 1)], zbuf.at[n].reshape(NY, CZ, CT, E).at[:, (1 - way) * (CZ - 1)],
                 (ix, step(iz, by, nz), it))
            )
        for way in (0, 1) if nx > 2 else (0,):
            by = 1 if way else -1
            moves.append(("x%d" % way, mine, xbuf.at[n, way], (step(ix, by, nx), iz, it)))
        copies = {}
        for number, (name, source, target, device) in enumerate(moves):
            copy = pltpu.make_async_remote_copy(
                src_ref=source, dst_ref=target,
                send_sem=send_sem.at[n, number], recv_sem=recv_sem.at[n, number],
                device_id=device, device_id_type=MESH,
            )
            copy.start()
            copies[name] = copy
        return copies

    def products(passes, fresh, merge=False):
        def body(c, carry):
            if fresh:
                sums = [jnp.zeros((8, 128), jnp.float32) for _ in range(4)]
            else:
                sums = [acc[i, c] for i in range(4)]
            for link, near in passes:
                for j in range(DOF // 8):
                    rows = pl.ds(8 * j, 8)
                    lr = links[link, 0, c, rows, :]
                    li = links[link, 1, c, rows, :]
                    if merge:
                        lr = lr + links[link + 1, 0, c, rows, :]
                        li = li + links[link + 1, 1, c, rows, :]
                        links[link, 0, c, rows, :] = lr
                        links[link, 1, c, rows, :] = li
                    for r in range(RHS):
                        vr = turned[near, pl.ds(2 * r * DOF + 8 * j, 8), :]
                        vi = turned[near, pl.ds((2 * r + 1) * DOF + 8 * j, 8), :]
                        sums[2 * r] = sums[2 * r] + lr * vr - li * vi
                        sums[2 * r + 1] = sums[2 * r + 1] + lr * vi + li * vr
            for i in range(4):
                acc[i, c] = sums[i]
            return carry

        lax.fori_loop(0, DOF, body, 0, unroll=2)

    lane8 = lax.broadcasted_iota(jnp.int32, (8, 128), 1)

    def split_links():
        inner = (lane8 // CT) % CZ == 0
        last = lane8 % CT == CT - 1

        def body(c, carry):
            for p in range(2):
                for j in range(DOF // 8):
                    rows = pl.ds(8 * j, 8)
                    up, down = links[5, p, c, rows, :], links[6, p, c, rows, :]
                    links[5, p, c, rows, :] = jnp.where(inner, up, down)
                    links[6, p, c, rows, :] = jnp.where(inner, down, up)
                    up, down = links[7, p, c, rows, :], links[8, p, c, rows, :]
                    links[9, p, c, rows, :] = jnp.where(last, up, down)
            return carry

        lax.fori_loop(0, DOF, body, 0, unroll=2)

    def fold(xs):
        low = row8 < 4
        ys = [
            jnp.where(low, xs[i], xs[i + 4]) + pltpu.roll(jnp.where(low, xs[i + 4], xs[i]), 4, 0)
            for i in range(4)
        ]
        low = row8 % 4 < 2
        zs = [
            jnp.where(low, ys[i] + pltpu.roll(ys[i], 6, 0), ys[i + 2] + pltpu.roll(ys[i + 2], 2, 0))
            for i in range(2)
        ]
        return jnp.where(
            row8 % 2 < 1, zs[0] + pltpu.roll(zs[0], 7, 0), zs[1] + pltpu.roll(zs[1], 1, 0)
        )

    def apply(n, copies):
        own = turned[0]
        turned[3] = pltpu.roll(own, S - CZ * CT, 1)
        turned[4] = pltpu.roll(own, CZ * CT, 1)
        turned[5] = jnp.where(in_z == 0, pltpu.roll(own, S - CT, 1), pltpu.roll(own, CT, 1))
        turned[7] = jnp.where(in_t == CT - 1, 0.0, pltpu.roll(own, S - 1, 1))
        turned[8] = jnp.where(in_t == 0, 0.0, pltpu.roll(own, 1, 1))
        if n == 0:
            for k in range(9):
                l_copies[k].wait()
            split_links()
        products(((0, 0), (3, 3), (4, 4)), True)
        products(((5, 5), (7, 7), (8, 8)), False)
        copies["x0"].wait_recv()
        turned[1] = xbuf[n, 0].T
        if nx > 2:
            copies["x1"].wait_recv()
            turned[2] = xbuf[n, 1].T
            products(((1, 1), (2, 2)), False)
        else:
            products(((1, 1),), False, n == 0)
        copies["z0"].wait_recv()
        copies["z1"].wait_recv()
        turned[6] = zbuf[n].T
        products(((6, 6),), False)
        copies["t0"].wait_recv()
        copies["t1"].wait_recv()
        edge = field.at[3]
        edge[pl.ds(CT - 1, NY * CZ, stride=CT), :] = tbuf[n, 0]
        edge[pl.ds(0, NY * CZ, stride=CT), :] = tbuf[n, 1]
        turned[9] = edge[...].T
        products(((9, 9),), False)
        for i in range(4):
            for c in range(0, DOF, 8):
                turned[0, pl.ds(i * DOF + c, 8), :] = fold([acc[i, c + j] for j in range(8)])
        field[n + 1] = turned[0].T

    field[3] = jnp.zeros((S, E), jnp.float32)
    first = halo(0)
    turned[0] = field[0].T
    apply(0, first)
    second = halo(1)
    apply(1, second)

    in_p = (lax.broadcasted_iota(jnp.int32, (S, E), 1) // DOF) % 2

    def aside(v):
        return jnp.where(in_p == 0, pltpu.roll(v, E - DOF, 1), -pltpu.roll(v, DOF, 1))

    def total(u, v):
        return jnp.sum((u * v).reshape(S // 8, 8, E), axis=0)

    k0, k1, k2 = field[0], field[1], field[2]
    z1, z2 = aside(k1), aside(k2)
    sums = [
        total(k0, k0), total(k1, k1), total(k2, k2), total(k0, k1), total(k0, z1),
        total(k0, k2), total(k0, z2),
    ]
    first_p = in_p[:8] == 0

    def both(v):
        return v + jnp.where(first_p, pltpu.roll(v, E - DOF, 1), pltpu.roll(v, DOF, 1))

    sums.append(jnp.where(first_p, both(total(k1, k2)), both(total(k1, z2))))
    part[...] = fold(sums)

    def exchange(count, target, sends, recvs, device):
        copies = []
        for delta in range(1, count):
            copies.append(
                pltpu.make_async_remote_copy(
                    src_ref=target.at[0], dst_ref=target.at[delta],
                    send_sem=sends.at[delta], recv_sem=recvs.at[delta],
                    device_id=device(delta), device_id_type=MESH,
                )
            )
        for copy in copies:
            copy.start()
        value = target[0]
        for copy in copies:
            copy.wait_recv()
        for delta in range(1, count):
            value = value + target[delta]
        return copies, value

    red1[0] = part[...]
    sent1, value = exchange(group, red1, s1_send, s1_recv, mate)
    red2[0] = value
    sent2, value = exchange(
        nt, red2, s2_send, s2_recv, lambda delta: (ix, iz, step(it, delta, nt))
    )
    quarter = lax.broadcasted_iota(jnp.int32, (8, 128), 1) // DOF
    sum00, sum01, sum10, sum11 = [
        jnp.sum(jnp.where(quarter == i, value, 0.0), axis=1, keepdims=True) for i in range(4)
    ]
    half = quarter < 2
    gram = jnp.where(half, sum00 + sum01, sum10 + sum11)
    g = [gram[i : i + 1] for i in range(7)]
    g.append(jnp.where(half, sum00, sum10)[7:8])
    g.append(jnp.where(half, sum01, sum11)[7:8])
    wa, wb = coefficients(g[0], g[1], g[2], (g[3], g[4]), (g[5], g[6]), (g[7], g[8]))

    def weighted(w, v, z):
        return w[0] * v - w[1] * z

    k0, k1, k2 = field[0], field[1], field[2]
    z0, z1, z2 = aside(k0), aside(k1), aside(k2)
    sol = weighted(wa, k0, z0) + weighted(wb, k1, z1)
    image = weighted(wa, k1, z1) + weighted(wb, k2, z2)
    sol_ref[0, 0, 0] = sol
    res_ref[0, 0, 0] = k0 - mass_shift * sol - image
    for copies in (first, second):
        for copy in copies.values():
            copy.wait_send()
    for copy in sent1 + sent2:
        copy.wait_send()


def deliver(a_ref, b_ref, sol_ref, res_ref):
    sol_ref[...] = a_ref[...]
    res_ref[...] = b_ref[...]


def shards(sizes, right_side, link_blocks):
    nx, nz, nt = sizes
    out = jax.ShapeDtypeStruct(right_side.shape, jnp.float32)
    f32 = jnp.float32
    moves = 6 if nx > 2 else 5
    held = pltpu.VMEM(right_side.shape, f32)
    results = pl.pallas_call(
        functools.partial(kernel, sizes),
        out_shape=(held, held),
        in_specs=[pl.BlockSpec(memory_space=pl.ANY)] * 2,
        out_specs=(pl.BlockSpec(memory_space=pltpu.VMEM),) * 2,
        scratch_shapes=[
            pltpu.VMEM((10, 2, DOF, DOF, S), f32),
            pltpu.VMEM((4, S, E), f32),
            pltpu.VMEM((2, 2, S, E), f32),
            pltpu.VMEM((2, S, E), f32),
            pltpu.VMEM((2, 2, NY * CZ, E), f32),
            pltpu.VMEM((2, 2, NY * CZ, E), f32),
            pltpu.VMEM((10, E, S), f32),
            pltpu.VMEM((4, DOF, 8, S), f32),
            pltpu.VMEM((8, 128), f32),
            pltpu.VMEM((nx * nz, 8, 128), f32),
            pltpu.VMEM((nt, 8, 128), f32),
            pltpu.SemaphoreType.DMA,
            pltpu.SemaphoreType.DMA((9,)),
            pltpu.SemaphoreType.DMA((2, moves)),
            pltpu.SemaphoreType.DMA((2, moves)),
            pltpu.SemaphoreType.DMA((nx * nz,)),
            pltpu.SemaphoreType.DMA((nx * nz,)),
            pltpu.SemaphoreType.DMA((nt,)),
            pltpu.SemaphoreType.DMA((nt,)),
        ],
        compiler_params=pltpu.CompilerParams(
            collective_id=0, has_side_effects=True, vmem_limit_bytes=56 * 1024 * 1024
        ),
    )(right_side, link_blocks)
    return pl.pallas_call(
        deliver,
        out_shape=(out, out),
        in_specs=[pl.BlockSpec(memory_space=pltpu.VMEM)] * 2,
        out_specs=(pl.BlockSpec(memory_space=pltpu.VMEM),) * 2,
    )(*[pltpu.with_memory_space_constraint(x, pltpu.VMEM) for x in results])


def solution(mesh):
    sizes = tuple(mesh.shape[name] for name in ("xy", "gz", "ta"))
    return jax.shard_map(
        functools.partial(shards, sizes),
        mesh=mesh,
        in_specs=(
            P("xy", "gz", "ta", None, None),
            P("xy", "gz", "ta", None, None, None, None, None),
        ),
        out_specs=(P("xy", "gz", "ta", None, None), P("xy", "gz", "ta", None, None)),
        check_vma=False,
    )
```

```python
import functools

import jax
import jax.numpy as jnp
from jax import lax
from jax.experimental import pallas as pl
from jax.experimental.pallas import tpu as pltpu
from jax.sharding import PartitionSpec as P

DOF = 32
RHS = 2
NY = 8
CZ = 2
CT = 8
S = 128
E = 128
MESH = pl.DeviceIdType.MESH

mass_shift = 4.0
epsilon = 1e-06


def cmul(a, b):
    return (a[0] * b[0] - a[1] * b[1], a[0] * b[1] + a[1] * b[0])


def conj(a):
    return (a[0], -a[1])


def cadd(a, b):
    return (a[0] + b[0], a[1] + b[1])


def csub(a, b):
    return (a[0] - b[0], a[1] - b[1])


def scale(a, x):
    return (a[0] * x, a[1] * x)


def size2(a):
    return a[0] * a[0] + a[1] * a[1]


def coefficients(g00, g11, g22, g01, g02, g12):
    beta2 = g00 + epsilon
    beta = jnp.sqrt(beta2)
    inv_beta2 = 1.0 / beta2
    h00 = scale((mass_shift * g00 + g01[0], g01[1]), inv_beta2)
    a = (mass_shift - h00[0], -h00[1])
    left = g11 + size2(a) * g00 + 2.0 * cmul(conj(a), g01)[0]
    h10_2 = jnp.maximum(left, 0.0) * inv_beta2 + epsilon
    h10 = jnp.sqrt(h10_2)
    a4 = (a[0] + mass_shift, a[1])
    a_4 = scale(a, mass_shift)
    top = cadd(cadd(g02, cmul(a4, g01)), scale(a_4, g00))
    h01 = scale(top, inv_beta2 / h10)
    low = cadd(cadd(g12, scale(a4, g11)), cmul(a_4, conj(g01)))
    h11 = scale(cadd(low, cmul(conj(a), top)), inv_beta2 / h10_2)
    p = csub(a4, h11)
    q = csub(csub(a_4, scale(h01, h10)), cmul(h11, a))
    left = g22 + size2(p) * g11 + size2(q) * g00
    left = left + 2.0 * (
        cmul(p, conj(g12))[0] + cmul(q, conj(g02))[0] + cmul(cmul(conj(q), p), g01)[0]
    )
    h21_2 = jnp.maximum(left, 0.0) * (inv_beta2 / h10_2) + epsilon
    m00 = size2(h00) + h10_2
    m01 = cadd(cmul(conj(h00), h01), scale(h11, h10))
    m11 = size2(h01) + size2(h11) + h21_2
    t0 = scale(conj(h00), beta)
    t1 = scale(conj(h01), beta)
    inv_l0 = 1.0 / jnp.sqrt(m00)
    l10 = scale(conj(m01), inv_l0)
    f0 = scale(t0, inv_l0)
    inv_d = 1.0 / (m11 - size2(l10))
    y1 = scale(csub(t1, cmul(l10, f0)), inv_d)
    y0 = scale(csub(f0, cmul(conj(l10), y1)), inv_l0)
    inv_beta = 1.0 / beta
    wb = scale(y1, inv_beta / h10)
    wa = cadd(scale(y0, inv_beta), cmul(wb, a))
    return wa, wb


def kernel(
    sizes, b_hbm, l_hbm, sol_ref, res_ref,
    links, field, xbuf, zbuf, tface, tbuf, turned, acc, red,
    b_sem, l_sem, send_sem, recv_sem, sum_send, sum_recv,
):
    nx, nz, nt = sizes
    total_count = nx * nz * nt
    ix, iz, it = lax.axis_index("xy"), lax.axis_index("gz"), lax.axis_index("ta")
    here = (ix * nz + iz) * nt + it

    def step(axis_value, by, count):
        return lax.rem(axis_value + (by + count), count)

    def mate(delta):
        other = lax.rem(here + delta, total_count)
        plane = other // nt
        return (plane // nz, lax.rem(plane, nz), lax.rem(other, nt))

    order = [0, 3, 4, 1, 2, 7, 8, 5, 6]
    b_copy = pltpu.make_async_copy(b_hbm.at[0, 0, 0], field.at[0], b_sem)
    b_copy.start()
    l_copies = {}
    for k in order:
        l_copies[k] = pltpu.make_async_copy(l_hbm.at[0, 0, 0, k], links.at[k], l_sem.at[k])
        l_copies[k].start()

    barrier = pltpu.get_barrier_semaphore()
    for delta in range(1, total_count):
        pl.semaphore_signal(barrier, inc=1, device_id=mate(delta), device_id_type=MESH)
    pl.semaphore_wait(barrier, total_count - 1)
    b_copy.wait()

    lane = lax.broadcasted_iota(jnp.int32, (S, E), 1)
    in_t = lane % CT
    in_z = (lane // CT) % CZ
    row8 = lax.broadcasted_iota(jnp.int32, (8, 128), 0)

    def halo(n):
        mine = field.at[n]
        tface[n, 0] = field[n, pl.ds(0, NY * CZ, stride=CT), :]
        tface[n, 1] = field[n, pl.ds(CT - 1, NY * CZ, stride=CT), :]
        tiles = mine.reshape(NY, CZ, CT, E)
        moves = []
        for way in (0, 1):
            by = 1 if way else -1
            moves.append(("t%d" % way, tface.at[n, way], tbuf.at[n, way], (ix, iz, step(it, by, nt))))
        for way in (0, 1):
            by = 1 if way else -1
            moves.append(
                ("z%d" % way, tiles.at[:, way * (CZ - 1)], zbuf.at[n].reshape(NY, CZ, CT, E).at[:, (1 - way) * (CZ - 1)],
                 (ix, step(iz, by, nz), it))
            )
        for way in (0, 1) if nx > 2 else (0,):
            by = 1 if way else -1
            moves.append(("x%d" % way, mine, xbuf.at[n, way], (step(ix, by, nx), iz, it)))
        copies = {}
        for number, (name, source, target, device) in enumerate(moves):
            copy = pltpu.make_async_remote_copy(
                src_ref=source, dst_ref=target,
                send_sem=send_sem.at[n, number], recv_sem=recv_sem.at[n, number],
                device_id=device, device_id_type=MESH,
            )
            copy.start()
            copies[name] = copy
        return copies

    def products(passes, fresh, merge=False):
        def body(c, carry):
            if fresh:
                sums = [jnp.zeros((8, 128), jnp.float32) for _ in range(4)]
            else:
                sums = [acc[i, c] for i in range(4)]
            for link, near in passes:
                for j in range(DOF // 8):
                    rows = pl.ds(8 * j, 8)
                    lr = links[link, 0, c, rows, :]
                    li = links[link, 1, c, rows, :]
                    if merge:
                        lr = lr + links[link + 1, 0, c, rows, :]
                        li = li + links[link + 1, 1, c, rows, :]
                        links[link, 0, c, rows, :] = lr
                        links[link, 1, c, rows, :] = li
                    for r in range(RHS):
                        vr = turned[near, pl.ds(2 * r * DOF + 8 * j, 8), :]
                        vi = turned[near, pl.ds((2 * r + 1) * DOF + 8 * j, 8), :]
                        sums[2 * r] = sums[2 * r] + lr * vr - li * vi
                        sums[2 * r + 1] = sums[2 * r + 1] + lr * vi + li * vr
            for i in range(4):
                acc[i, c] = sums[i]
            return carry

        lax.fori_loop(0, DOF, body, 0, unroll=2)

    lane8 = lax.broadcasted_iota(jnp.int32, (8, 128), 1)

    def split_links():
        inner = (lane8 // CT) % CZ == 0
        last = lane8 % CT == CT - 1

        def body(c, carry):
            for p in range(2):
                for j in range(DOF // 8):
                    rows = pl.ds(8 * j, 8)
                    up, down = links[5, p, c, rows, :], links[6, p, c, rows, :]
                    links[5, p, c, rows, :] = jnp.where(inner, up, down)
                    links[6, p, c, rows, :] = jnp.where(inner, down, up)
                    up, down = links[7, p, c, rows, :], links[8, p, c, rows, :]
                    links[9, p, c, rows, :] = jnp.where(last, up, down)
            return carry

        lax.fori_loop(0, DOF, body, 0, unroll=2)

    def fold(xs):
        low = row8 < 4
        ys = [
            jnp.where(low, xs[i], xs[i + 4]) + pltpu.roll(jnp.where(low, xs[i + 4], xs[i]), 4, 0)
            for i in range(4)
        ]
        low = row8 % 4 < 2
        zs = [
            jnp.where(low, ys[i] + pltpu.roll(ys[i], 6, 0), ys[i + 2] + pltpu.roll(ys[i + 2], 2, 0))
            for i in range(2)
        ]
        return jnp.where(
            row8 % 2 < 1, zs[0] + pltpu.roll(zs[0], 7, 0), zs[1] + pltpu.roll(zs[1], 1, 0)
        )

    def apply(n, copies):
        own = turned[0]
        turned[3] = pltpu.roll(own, S - CZ * CT, 1)
        turned[4] = pltpu.roll(own, CZ * CT, 1)
        turned[5] = jnp.where(in_z == 0, pltpu.roll(own, S - CT, 1), pltpu.roll(own, CT, 1))
        turned[7] = jnp.where(in_t == CT - 1, 0.0, pltpu.roll(own, S - 1, 1))
        turned[8] = jnp.where(in_t == 0, 0.0, pltpu.roll(own, 1, 1))
        if n == 0:
            for k in range(9):
                l_copies[k].wait()
            split_links()
        products(((0, 0), (3, 3), (4, 4)), True)
        products(((5, 5), (7, 7), (8, 8)), False)
        copies["x0"].wait_recv()
        turned[1] = xbuf[n, 0].T
        if nx > 2:
            copies["x1"].wait_recv()
            turned[2] = xbuf[n, 1].T
            products(((1, 1), (2, 2)), False)
        else:
            products(((1, 1),), False, n == 0)
        copies["z0"].wait_recv()
        copies["z1"].wait_recv()
        turned[6] = zbuf[n].T
        products(((6, 6),), False)
        copies["t0"].wait_recv()
        copies["t1"].wait_recv()
        edge = field.at[3]
        edge[pl.ds(CT - 1, NY * CZ, stride=CT), :] = tbuf[n, 0]
        edge[pl.ds(0, NY * CZ, stride=CT), :] = tbuf[n, 1]
        turned[9] = edge[...].T
        products(((9, 9),), False)
        for i in range(4):
            for c in range(0, DOF, 8):
                turned[0, pl.ds(i * DOF + c, 8), :] = fold([acc[i, c + j] for j in range(8)])
        field[n + 1] = turned[0].T

    field[3] = jnp.zeros((S, E), jnp.float32)
    first = halo(0)
    turned[0] = field[0].T
    apply(0, first)
    second = halo(1)
    apply(1, second)

    in_p = (lax.broadcasted_iota(jnp.int32, (S, E), 1) // DOF) % 2

    def aside(v):
        return jnp.where(in_p == 0, pltpu.roll(v, E - DOF, 1), -pltpu.roll(v, DOF, 1))

    def total(u, v):
        return jnp.sum((u * v).reshape(S // 8, 8, E), axis=0)

    k0, k1, k2 = field[0], field[1], field[2]
    z1, z2 = aside(k1), aside(k2)
    sums = [
        total(k0, k0), total(k1, k1), total(k2, k2), total(k0, k1), total(k0, z1),
        total(k0, k2), total(k0, z2),
    ]
    first_p = in_p[:8] == 0

    def both(v):
        return v + jnp.where(first_p, pltpu.roll(v, E - DOF, 1), pltpu.roll(v, DOF, 1))

    sums.append(jnp.where(first_p, both(total(k1, k2)), both(total(k1, z2))))
    lanes = fold(sums)
    for width in (16, 8, 4):
        low = lane8 % (2 * width) < width
        lanes = lanes + jnp.where(
            low, pltpu.roll(lanes, 128 - width, 1), pltpu.roll(lanes, width, 1)
        )
    seat = (lane8 % DOF) // 4 == row8
    red[0] = jnp.sum(jnp.where(seat, lanes, 0.0), axis=0, keepdims=True)
    sent = []
    for delta in range(1, total_count):
        copy = pltpu.make_async_remote_copy(
            src_ref=red.at[0], dst_ref=red.at[delta],
            send_sem=sum_send.at[delta], recv_sem=sum_recv.at[delta],
            device_id=mate(delta), device_id_type=MESH,
        )
        copy.start()
        sent.append(copy)
    for copy in sent:
        copy.wait_recv()
    value = jnp.where(seat, jnp.sum(red[...], axis=0), 0.0)
    quarter = lax.broadcasted_iota(jnp.int32, (8, 128), 1) // DOF
    sum00, sum01, sum10, sum11 = [
        jnp.sum(jnp.where(quarter == i, value, 0.0), axis=1, keepdims=True) for i in range(4)
    ]
    half = quarter < 2
    gram = jnp.where(half, sum00 + sum01, sum10 + sum11)
    g = [gram[i : i + 1] for i in range(7)]
    g.append(jnp.where(half, sum00, sum10)[7:8])
    g.append(jnp.where(half, sum01, sum11)[7:8])
    wa, wb = coefficients(g[0], g[1], g[2], (g[3], g[4]), (g[5], g[6]), (g[7], g[8]))

    def weighted(w, v, z):
        return w[0] * v - w[1] * z

    k0, k1, k2 = field[0], field[1], field[2]
    z0, z1, z2 = aside(k0), aside(k1), aside(k2)
    sol = weighted(wa, k0, z0) + weighted(wb, k1, z1)
    image = weighted(wa, k1, z1) + weighted(wb, k2, z2)
    sol_ref[0, 0, 0] = sol
    res_ref[0, 0, 0] = k0 - mass_shift * sol - image
    for copies in (first, second):
        for copy in copies.values():
            copy.wait_send()
    for copy in sent:
        copy.wait_send()


def deliver(a_ref, b_ref, sol_ref, res_ref):
    sol_ref[...] = a_ref[...]
    res_ref[...] = b_ref[...]


def shards(sizes, right_side, link_blocks):
    nx, nz, nt = sizes
    out = jax.ShapeDtypeStruct(right_side.shape, jnp.float32)
    f32 = jnp.float32
    moves = 6 if nx > 2 else 5
    held = pltpu.VMEM(right_side.shape, f32)
    results = pl.pallas_call(
        functools.partial(kernel, sizes),
        out_shape=(held, held),
        in_specs=[pl.BlockSpec(memory_space=pl.ANY)] * 2,
        out_specs=(pl.BlockSpec(memory_space=pltpu.VMEM),) * 2,
        scratch_shapes=[
            pltpu.VMEM((10, 2, DOF, DOF, S), f32),
            pltpu.VMEM((4, S, E), f32),
            pltpu.VMEM((2, 2, S, E), f32),
            pltpu.VMEM((2, S, E), f32),
            pltpu.VMEM((2, 2, NY * CZ, E), f32),
            pltpu.VMEM((2, 2, NY * CZ, E), f32),
            pltpu.VMEM((10, E, S), f32),
            pltpu.VMEM((4, DOF, 8, S), f32),
            pltpu.VMEM((nx * nz * nt, 1, 128), f32),
            pltpu.SemaphoreType.DMA,
            pltpu.SemaphoreType.DMA((9,)),
            pltpu.SemaphoreType.DMA((2, moves)),
            pltpu.SemaphoreType.DMA((2, moves)),
            pltpu.SemaphoreType.DMA((nx * nz * nt,)),
            pltpu.SemaphoreType.DMA((nx * nz * nt,)),
        ],
        compiler_params=pltpu.CompilerParams(
            collective_id=0, has_side_effects=True, vmem_limit_bytes=56 * 1024 * 1024
        ),
    )(right_side, link_blocks)
    return pl.pallas_call(
        deliver,
        out_shape=(out, out),
        in_specs=[pl.BlockSpec(memory_space=pltpu.VMEM)] * 2,
        out_specs=(pl.BlockSpec(memory_space=pltpu.VMEM),) * 2,
    )(*[pltpu.with_memory_space_constraint(x, pltpu.VMEM) for x in results])


def solution(mesh):
    sizes = tuple(mesh.shape[name] for name in ("xy", "gz", "ta"))
    return jax.shard_map(
        functools.partial(shards, sizes),
        mesh=mesh,
        in_specs=(
            P("xy", "gz", "ta", None, None),
            P("xy", "gz", "ta", None, None, None, None, None),
        ),
        out_specs=(P("xy", "gz", "ta", None, None), P("xy", "gz", "ta", None, None)),
        check_vma=False,
    )
```
